256 devices in a mesh: row: 16 (over x, z_hi), col: 8 (over y, core), ga: 2 (over z_lo).
Axes of the slice: x: 4, y: 4, z: 8 (z_hi: 4, z_lo: 2; z = z_hi * 2 + z_lo), core: 2. Of those that a mesh axis runs over, the one named last changes fastest.
Arguments:
- pair_density: float32 [512, 24, 3072], P('row', None, 'ga'), may hold values from -6 to 6
- coulomb: float32 [3072], P('ga'), may hold values from 0.1 to 2
Outputs:
- kernel: float32 [12288, 12288], P('row', 'col')
The draws below stay inside these ranges and needn't reach their ends.
All inputs are finite; a program needn't handle non-finite values.
Results may differ from the reference program's by a relative error of at most 0.00011.
Values sent between devices are 32-bit elements; how exact they have to be, the bound alone decides.
No kernel may reach another device: no remote copies, remote signals or barrier semaphores. Data moves between devices by JAX's collectives and lax.ppermute only.
A program may use at most 64 MiB of HBM per device.

```python
import math
import jax
import jax.numpy as jnp
from jax import lax

NG = 3072
NK = 512
NVC = 24
N_ROW = 16
N_COL = 8


def level_of(own_key, extent, cuts, low, top_value):
    gain, own = 1.0, jax.random.fold_in(own_key, 6)
    for position, blocks in cuts:
        steps = jnp.exp(jax.random.uniform(jax.random.fold_in(own, position), (blocks,), jnp.float32, low / len(cuts), top_value / len(cuts)))
        gain = gain * jnp.repeat(steps, extent[position] // blocks).reshape([-1 if axis == position else 1 for axis in range(len(extent))])
    return gain


def bell_draw(rng, shape, spread, limit, split=(), kind=jnp.bfloat16):
    drawn = spread * jax.random.normal(rng, shape, jnp.float32)
    if split:
        drawn = drawn * level_of(rng, shape, split, -0.22, 0.18)
    return jnp.clip(drawn, -limit, limit).astype(kind)


def setup_inputs(seed: int = 0) -> dict:
    key_of = jax.random.split(jax.random.key(seed), 3)
    pair_density = bell_draw(key_of[0], (NK, NVC, NG), 1.0, 6.0, ((0, 16), (2, 2)), jnp.float32)
    coulomb = jnp.clip(jnp.exp(math.log(2.0) - 2.9957323 * jax.random.uniform(key_of[1], (NG,), jnp.float32) ** level_of(key_of[1], (NG,), ((0, 2),), -0.2, 0.2)), 0.1, 2.0)
    return {"pair_density": pair_density, "coulomb": coulomb}


def contract(left_rows, right_rows):
    return lax.dot_general(left_rows, right_rows, (((1,), (1,)), ((), ())), precision=lax.Precision.HIGHEST, preferred_element_type=jnp.float32)


def reference(pair_density, coulomb):
    row_order = jnp.arange(NK, dtype=jnp.int32).reshape(NK // N_ROW, N_ROW).T.reshape(-1)
    col_order = jnp.arange(NK, dtype=jnp.int32).reshape(NK // N_COL, N_COL).T.reshape(-1)
    left = pair_density[row_order]
    right = pair_density[col_order]
    bands = pair_density.shape[1]
    g_width = pair_density.shape[2]
    weighted = left.reshape(NK * bands, g_width) * (2.0 * coulomb)[None, :]
    exchange = contract(weighted, right.reshape(NK * bands, g_width))
    return exchange / jnp.float32(NK)
```

```python
import functools

import jax
import jax.numpy as jnp
from jax import lax
from jax.experimental import pallas as pl
from jax.experimental.pallas import tpu as pltpu
from jax.sharding import PartitionSpec as P


N_X, N_Z = 4, 8
PLANE = ("row", "ga")
LANES_A = 512
LANES_B = 1536 - LANES_A
STEPS = (0, -1, 1, 2)
GROUPS = ((0,), (-1, 1), (-2, 2), (-3, 3, 4))


def plane_permute(value, target):
    pairs = []
    for x in range(N_X):
        for z in range(N_Z):
            tx, tz = target(x, z)
            pairs.append((x * N_Z + z, tx % N_X * N_Z + tz % N_Z))
    return lax.ppermute(value, PLANE, pairs)


def shift(value, dx, dz):
    return plane_permute(value, lambda x, z: (x + dx, z + dz))


def shift_y(value, dy):
    pairs = [(y * 2 + c, (y + dy) % 4 * 2 + c) for y in range(4) for c in range(2)]
    return lax.ppermute(value, "col", pairs)


def gather_part_a(own):
    minus = shift(own, 1, 0)
    plus = shift(own, -1, 0)
    low = shift(minus[:48], 1, 0)
    high = shift(plus[48:], -1, 0)
    here = jnp.concatenate([own, minus, plus, low, high], 0)
    got = {0: [here]}
    down, up = here, here
    for n in (1, 2, 3):
        down = shift(down, 0, 1)
        up = shift(up, 0, -1)
        got[-n], got[n] = [down], [up]
    got[4] = [shift(down[:192], 0, 1), shift(up[192:], 0, -1)]
    return got


def gather_part_b(own):
    blocks = {0: [own]}
    down, up = own, own
    for n in (1, 2, 3):
        down = shift(down, 0, 1)
        up = shift(up, 0, -1)
        blocks[-n], blocks[n] = [down], [up]
    blocks[4] = [shift(down[:48], 0, 1), shift(up[48:], 0, -1)]
    sent, minus, plus = [], [], []
    for k, group in enumerate(GROUPS):
        parts = [piece for d in group for piece in blocks[d]]
        mine = jnp.concatenate(parts, 0) if len(parts) > 1 else parts[0]
        sent.append(mine)
        ahead, behind = mine, mine
        if k:
            rows = len(GROUPS[k - 1]) * 96
            ahead = jnp.concatenate([mine, minus[-1][: rows // 2]], 0)
            behind = jnp.concatenate([mine, plus[-1][rows // 2 : rows]], 0)
        minus.append(shift(ahead, 1, 0))
        plus.append(shift(behind, -1, 0))
    rows = len(GROUPS[-1]) * 96
    far_low = shift(minus[-1][: rows // 2], 1, 0)
    far_high = shift(plus[-1][rows // 2 : rows], -1, 0)
    return sent, minus, plus, far_low, far_high


def gather_rows(pair_density, doubled):
    row, col = lax.axis_index("row"), lax.axis_index("col")
    x, h, y, core = row // 4, row % 4, col // 2, col % 2
    piece = lax.dynamic_slice(pair_density, (16 * core, 0, 384 * y), (16, 24, 384))
    weighted = piece * lax.dynamic_slice(doubled, (384 * y,), (384,))
    by_x = weighted.reshape(4, 96, 384)

    def part(value, index, axis):
        return lax.dynamic_index_in_dim(value, index % 4, axis, keepdims=False)

    got = [part(by_x, x, 0)]
    got += [shift(part(by_x, x - d, 0), -d, 0) for d in STEPS[1:]]
    by_h = jnp.stack(got).reshape(4, 4, 24, 384)
    got = [part(by_h, h, 1)]
    got += [shift(part(by_h, h - d, 1), 0, -2 * d) for d in STEPS[1:]]
    near = jnp.stack(got).reshape(384, 384)
    partner = plane_permute(near, lambda x, z: (x, z ^ 1))
    own = jnp.concatenate([near, partner], 0)
    minus = shift_y(own, 1)
    plus = shift_y(own, -1)
    low = shift_y(minus[:384], 1)
    high = shift_y(plus[384:], -1)
    mine = jnp.concatenate([own, minus, plus, low, high], 0)
    other = lax.ppermute(mine, "col", [(i, i ^ 1) for i in range(8)])
    return mine, other


def b_pieces():
    table = {}
    for k, group in enumerate(GROUPS):
        rows = 96 * len(group)
        for n, d in enumerate(group):
            first, last = 96 * n, 96 * n + 96
            pieces = [(("sent", k), first, 96), (("minus", k), first, 96), (("plus", k), first, 96)]
            for kind, low, high in (("minus", 0, rows // 2), ("plus", rows // 2, rows)):
                a, b = max(first, low), min(last, high)
                if a < b:
                    if k + 1 < len(GROUPS):
                        base = 96 * len(GROUPS[k + 1])
                        pieces.append(((kind, k + 1), base + a - low, b - a))
                    else:
                        pieces.append((("far_" + kind, 0), a - low, b - a))
            table[d] = pieces
    return table


def panel_kernel(order, plan, n_in, where, mine, other, *refs):
    inputs, (out, rows_f, rows_hi, rows_lo, slab_a, slab_b, acc, sem_r, sem_a, sem_b) = refs[:n_in], refs[n_in:]
    x, h, g, y, core = (where[i] for i in range(5))

    def start_rows(i, carry):
        rel = lax.rem(i, 32)
        y_rel = lax.div(i, 32)
        y_to = lax.rem(y + jnp.where(y_rel == 1, 3, jnp.where(y_rel == 2, 1, jnp.where(y_rel == 3, 2, 0))), 4)
        parity, h_rel, x_rel = lax.div(rel, 16), lax.rem(lax.div(rel, 4), 4), lax.rem(rel, 4)

        def step(v):
            return jnp.where(v == 1, 3, jnp.where(v == 2, 1, jnp.where(v == 3, 2, 0)))

        r0 = lax.rem(x + step(x_rel), 4) * 4 + lax.rem(h + step(h_rel), 4)
        g0 = lax.rem(g + parity, 2)
        lanes = pl.ds(pl.multiple_of(y_to * 384, 128), 384)
        source = pl.ds(pl.multiple_of(i * 24, 8), 24)
        for ref, half in ((mine, core), (other, 1 - core)):
            target = pl.ds(pl.multiple_of(r0 * 48 + half * 24, 8), 24)
            pltpu.make_async_copy(ref.at[source, :], rows_f.at[g0, target, lanes], sem_r).start()
        return carry

    lax.fori_loop(0, 128, start_rows, 0)
    for n, d in enumerate(order):
        for slab, sem, pieces in ((slab_a, sem_a, plan["a"][d]), (slab_b, sem_b, plan["b"][d])):
            to = 0
            for ref, first, count in pieces:
                pltpu.make_async_copy(
                    inputs[ref].at[pl.ds(first, count), :], slab.at[n, pl.ds(to, count), :], sem.at[n]
                ).start()
                to += count
    pltpu.make_async_copy(rows_f, rows_f, sem_r).wait()
    for half in range(2):
        for part in range(4):
            span = pl.ds(part * 192, 192)
            value = rows_f[half, span, :]
            top = value.astype(jnp.bfloat16)
            rows_hi[half, span, :] = top
            rows_lo[half, span, :] = (value - top.astype(jnp.float32)).astype(jnp.bfloat16)

    def product(block, half, lanes):
        top = block.astype(jnp.bfloat16)
        rest = (block - top.astype(jnp.float32)).astype(jnp.bfloat16)
        hi, lo = rows_hi[half, :, lanes], rows_lo[half, :, lanes]

        def dot(a, b):
            return lax.dot_general(a, b, (((1,), (1,)), ((), ())), preferred_element_type=jnp.float32)

        return dot(top, hi) + dot(rest, hi) + dot(top, lo)

    for n, d in enumerate(order):
        pltpu.make_async_copy(slab_a.at[n], slab_a.at[n], sem_a.at[n]).wait()
        pltpu.make_async_copy(slab_b.at[n], slab_b.at[n], sem_b.at[n]).wait()
    z = 2 * h + g
    for parity in range(2):
        half = lax.rem(g + parity, 2)

        def job(n, carry, parity=parity, half=half):
            offset = 2 * n + parity
            zh = lax.div(lax.rem(z + offset, 8), 2)
            value = product(slab_a[offset], half, slice(0, LANES_A))
            value += product(slab_b[offset], half, slice(LANES_A, 1536))
            for i, dx in enumerate(STEPS):
                to = pl.multiple_of((lax.rem(x + dx + 4, 4) * 4 + zh) * 96, 8)
                piece = value[96 * i : 96 * i + 96]
                if parity:
                    piece = piece + acc[pl.ds(to, 96), :]
                acc[pl.ds(to, 96), :] = piece
            return carry

        lax.fori_loop(0, 4, job, 0)
    for n in range(12):
        span = slice(128 * n, 128 * n + 128)
        out[:, span] = acc[span, :].T * jnp.float32(1.0 / 512)


def panel(mine, other, part_a, part_b, where):
    sent, minus, plus, far_low, far_high = part_b
    order = (0, 1, 2, 3, 4, -3, -2, -1)
    inputs, index = [], {}

    def use(key, value):
        index[key] = len(inputs)
        inputs.append(value)

    for d in order:
        for n, value in enumerate(part_a[d]):
            use(("a", d, n), value)
    for k in range(len(GROUPS)):
        use(("sent", k), sent[k])
        use(("minus", k), minus[k])
        use(("plus", k), plus[k])
    use(("far_minus", 0), far_low)
    use(("far_plus", 0), far_high)
    plan = {
        "a": {d: [(index[("a", d, n)], 0, v.shape[0]) for n, v in enumerate(part_a[d])] for d in order},
        "b": {d: [(index[key], first, count) for key, first, count in p] for d, p in b_pieces().items()},
    }
    anywhere = pl.BlockSpec(memory_space=pl.ANY)
    return pl.pallas_call(
        functools.partial(panel_kernel, order, plan, len(inputs)),
        out_shape=jax.ShapeDtypeStruct((768, 1536), jnp.float32),
        in_specs=[pl.BlockSpec(memory_space=pltpu.SMEM)] + [anywhere] * (2 + len(inputs)),
        out_specs=pl.BlockSpec(memory_space=pltpu.VMEM),
        scratch_shapes=[
            pltpu.VMEM((2, 768, 1536), jnp.float32),
            pltpu.VMEM((2, 768, 1536), jnp.bfloat16),
            pltpu.VMEM((2, 768, 1536), jnp.bfloat16),
            pltpu.VMEM((8, 384, LANES_A), jnp.float32),
            pltpu.VMEM((8, 384, LANES_B), jnp.float32),
            pltpu.VMEM((1536, 768), jnp.float32),
            pltpu.SemaphoreType.DMA,
            pltpu.SemaphoreType.DMA((8,)),
            pltpu.SemaphoreType.DMA((8,)),
        ],
        compiler_params=pltpu.CompilerParams(vmem_limit_bytes=60 * 1024 * 1024),
        cost_estimate=pl.CostEstimate(flops=22_000_000_000, bytes_accessed=40_000_000, transcendentals=0),
        name="panel",
    )(where, mine, other, *inputs)


def local(pair_density, coulomb):
    row, col, ga = (lax.axis_index(a) for a in ("row", "col", "ga"))
    where = jnp.stack([row // 4, row % 4, ga, col // 2, col % 2]).astype(jnp.int32)
    mine, other = gather_rows(pair_density, 2.0 * coulomb)
    grouped = pair_density.reshape(4, 8, 24, 1536)
    own = lax.dynamic_index_in_dim(grouped, col, 1, keepdims=False).reshape(96, 1536)
    part_a = gather_part_a(own[:, :LANES_A])
    part_b = gather_part_b(own[:, LANES_A:])
    return panel(mine, other, part_a, part_b, where)


def solution(mesh):
    placed = (P("row", None, "ga"), P("ga"))
    return jax.shard_map(
        local, mesh=mesh, in_specs=placed, out_specs=P("row", "col"), check_vma=False
    )
```
